256 devices in a mesh: visit: 8 (over z), bulk: 32 (over x, y, core).
Axes of the slice: x: 4, y: 4, z: 8, core: 2. Of those that a mesh axis runs over, the one named last changes fastest.
Arguments:
- piece_flux: float32 [8, 32, 32, 128, 128], P('visit', 'bulk'), may hold values from -6 to 6
- piece_ivar: float32 [8, 32, 32, 128, 128], P('visit', 'bulk'), may hold values from 0.5 to 8
- warp_rows: float32 [8, 32, 32, 128, 128], P('visit', 'bulk'), may hold values from 0 to 1, as said below
- warp_cols: float32 [8, 32, 32, 128, 128], P('visit', 'bulk'), may hold values from 0 to 1, as said below
- piece_owner: int32 [8, 32, 32, 1], P('visit', 'bulk'), may hold values from 0 to 31; in each aligned block of 32 rows (0 to 31, 32 to 63, ..., all dimensions but the last counted through in order) at most 2 rows name the same one
- piece_slot: int32 [8, 32, 32], P('visit', 'bulk'), may hold values from 0 to 15
- piece_extent: int32 [8, 32, 32, 2], P('visit', 'bulk'), may hold values from 64 to 128
- basis: float32 [4, 128, 128], replicated, may hold values from -0.046875 to 0.046875
- coeffs: float32 [8, 4], P('visit'), may hold values from -4 to 4
Outputs:
- coadd: float32 [8192, 1024], P('bulk', 'visit')
- weight_map: float32 [8192, 1024], P('bulk', 'visit')
The draws below stay inside these ranges and needn't reach their ends.
Inputs may be any that keep to these rules, and one draw needn't show every extreme that they name: `piece_owner`: among the pieces on one device, no owner is named by more than 2 pieces, a bound that some block reaches. `warp_rows`: entries are nonnegative and each row sums to one. `warp_cols`: entries are nonnegative and each row sums to one.
All inputs are finite; a program needn't handle non-finite values.
Results may differ from the reference program's by a relative error of at most 0.0003.
Values sent between devices are 32-bit elements; how exact they have to be, the bound alone decides.
A program may use at most 128 MiB of HBM per device.

```python
import math
import jax
import jax.numpy as jnp
import numpy as np
from jax import lax

S = 128
HALO = 64
BR = 2
BC = 8
CAP = 2
BASES = 4
VISITS = 8
OWNERS = 32
PIECES_DEV = 32
COLS = 1024
NROWS = 8192
KS = 128


def dense_warp(key):
    full_shape = (VISITS, OWNERS, PIECES_DEV, S, S)
    key_diag, key_side = jax.random.split(key)
    positions = jnp.arange(S, dtype=jnp.int32)
    on_diag = positions[:, None] == positions[None, :]
    diagonal = jax.random.uniform(key_diag, full_shape, jnp.float32, 1.5, 2.5)
    side_vals = jax.random.uniform(key_side, full_shape, jnp.float32, 0.0, 2.0 / S)
    matrix = jnp.where(on_diag, diagonal, side_vals)
    return matrix / jnp.sum(matrix, axis=-1, keepdims=True)


def draw_warp_rows(key, part):
    return dense_warp(jax.random.fold_in(key, 11))


def draw_warp_cols(key, part):
    return dense_warp(jax.random.fold_in(key, 23))


def set_ends(values, key, least, largest):
    longest = values.shape.index(max(values.shape))
    spots = []
    for shift in (0, 1):
        where = [jax.random.randint(jax.random.fold_in(key, axis), (), 0, length) for axis, length in enumerate(values.shape)]
        where[longest] = (where[longest] + shift) % values.shape[longest]
        spots.append(tuple(where))
    return values.at[spots[0]].set(least).at[spots[1]].set(largest)


def block_scale(key, dims, cuts, smallest, high):
    level = 1.0
    for dim, blocks in cuts:
        draws = jax.random.uniform(jax.random.fold_in(jax.random.fold_in(key, 6), dim), (blocks,), jnp.float32, smallest / len(cuts), high / len(cuts))
        level = level * jnp.repeat(jnp.exp(draws), dims[dim] // blocks).reshape((-1,) + (1,) * (len(dims) - 1 - dim))
    return level


def deal_out(stream_key, own, number, rows, amount, top, limit, slope):
    sequence = jax.random.permutation(stream_key, amount)
    packed, usual = portions_of(amount, rows * top, limit, slope, True), portions_of(amount, rows * top, limit, slope, False)
    places = jnp.arange(amount)

    def named(lengths, rotation):
        used = int((lengths > 0).sum())
        fixed = max(1, used // 4)
        moved = fixed + (places - fixed + rotation * (used - fixed)) % max(1, amount - fixed)
        return jnp.zeros((amount,), jnp.int32).at[sequence[jnp.where(places < fixed, places, moved)]].set(jnp.asarray(lengths, jnp.int32))

    lengths = jnp.where(number % 4 == 0, named(packed, number // 4), named(usual, number - number // 4 - 1))
    mixed = jax.random.permutation(jax.random.fold_in(own, 3), amount)
    source_of, sink = mixed[0:amount // 2 * 2:2], mixed[1:amount // 2 * 2:2]
    margin = jnp.minimum(lengths[source_of] - 1, limit - lengths[sink]) // 2
    margin = jnp.where((source_of == sequence[0]) | (sink == sequence[0]) | (lengths[sink] == 0), 0, jnp.maximum(margin, 0))
    moved = jax.random.randint(jax.random.fold_in(own, 4), (amount // 2,), 0, 1 << 20) % (margin + 1)
    lengths = lengths.at[source_of].add(-moved).at[sink].add(moved)
    members = jnp.searchsorted(jnp.cumsum(lengths), jnp.arange(rows * top), side="right").astype(jnp.int32)
    table = members.reshape(top, rows).T
    table = table[jax.random.permutation(jax.random.fold_in(own, 1), rows)]
    rotation = jax.random.randint(jax.random.fold_in(own, 2), (rows, 1), 0, top)
    return jnp.take_along_axis(table, (jnp.arange(top)[None, :] + rotation) % top, axis=1)


def portions_of(amount, total, reach, skew, full):
    portions = [(1 << 20) // math.isqrt(grade ** skew) + 1 for grade in range(1, amount + 1)]
    largest = reach if full else min(reach, max(-(-total // amount), total * portions[0] // sum(portions)))
    least = 1 if total - largest >= amount - 1 else 0
    counts, surplus = [largest] + [least] * (amount - 1), total - largest - least * (amount - 1)
    while surplus > 0:
        free = [i for i in range(1, amount) if counts[i] < largest] or [i for i in range(1, amount) if counts[i] < reach]
        pool, remaining = sum([portions[i] for i in free]), surplus
        for i in free:
            more = min(reach - counts[i], max(1, remaining * portions[i] // pool), surplus)
            counts[i] = counts[i] + more
            surplus = surplus - more
    return np.array(counts)


def centred(key, shape, deviation, limit, cuts=(), kind=jnp.bfloat16):
    factor_of = block_scale(key, shape, cuts, -0.22, 0.18) if cuts else 1.0
    drawn = jax.random.normal(key, shape, jnp.float32) * deviation * factor_of
    return jnp.minimum(jnp.maximum(drawn, -limit), limit).astype(kind)


def setup_inputs(seed: int = 0) -> dict:
    splits = jax.random.split(jax.random.key(seed), 10)
    piece_flux = centred(splits[0], (VISITS, OWNERS, PIECES_DEV, S, S), 1.0, 6.0, ((0, 8), (1, 32)), jnp.float32)
    piece_ivar = jnp.clip(jnp.exp(math.log(8.0) - 2.7725887 * jax.random.uniform(splits[1], (VISITS, OWNERS, PIECES_DEV, S, S), jnp.float32) ** block_scale(splits[1], (VISITS, OWNERS, PIECES_DEV, S, S), ((0, 8), (1, 32)), -0.2, 0.2)), 0.5, 8.0)
    warp_rows = draw_warp_rows(jax.random.fold_in(splits[9], 71), 0)
    warp_cols = draw_warp_cols(jax.random.fold_in(splits[9], 71), 0)
    piece_owner_keys = jax.random.split(jax.random.fold_in(splits[4], 1), VISITS * OWNERS * PIECES_DEV // PIECES_DEV)
    piece_owner_turns = jax.random.permutation(jax.random.fold_in(splits[4], 3), VISITS * OWNERS * PIECES_DEV // PIECES_DEV)
    piece_owner = jax.vmap(lambda own, number: deal_out(jax.random.fold_in(splits[4], 2), own, number, PIECES_DEV, OWNERS, 1, CAP, 2))(piece_owner_keys, piece_owner_turns).reshape((VISITS, OWNERS, PIECES_DEV, 1))
    piece_slot = set_ends(jax.random.randint(splits[5], (VISITS, OWNERS, PIECES_DEV), 0, BR * BC), jax.random.fold_in(splits[5], 1), 0, (BR * BC) - 1).astype(jnp.int32)
    piece_extent = set_ends(jax.random.randint(splits[6], (VISITS, OWNERS, PIECES_DEV, 2), S // 2, S + 1), jax.random.fold_in(splits[6], 1), S // 2, S).astype(jnp.int32)
    basis = centred(splits[7], (BASES, KS, KS), (KS * KS) ** -0.5, 0.046875, (), jnp.float32)
    coeffs = centred(splits[8], (VISITS, BASES), 1.0, 4.0, ((0, 8),), jnp.float32)
    return dict(piece_flux=piece_flux, piece_ivar=piece_ivar, warp_rows=warp_rows, warp_cols=warp_cols, piece_owner=piece_owner, piece_slot=piece_slot, piece_extent=piece_extent, basis=basis, coeffs=coeffs)


HIGHEST_PREC = lax.Precision.HIGHEST


def warp_pieces(flux_data, ivar_data, row_maps, col_maps, extent):
    positions = jnp.arange(flux_data.shape[-1], dtype=jnp.int32)
    row_ok = positions[None, :, None] < extent[:, 0][:, None, None]
    col_ok = positions[None, None, :] < extent[:, 1][:, None, None]
    valid_mask = jnp.where(row_ok & col_ok, 1.0, 0.0).astype(flux_data.dtype)
    weighted = valid_mask * ivar_data
    planes = jnp.stack([weighted * flux_data, weighted], axis=1)
    inner = jnp.einsum("qcij,qkj->qcik", planes, col_maps, precision=HIGHEST_PREC)
    return jnp.einsum("qij,qcjk->qcik", row_maps, inner, precision=HIGHEST_PREC)


def match_psf(visit_image, kernel):
    row_total = visit_image.shape[0] + 2 * HALO
    col_total = visit_image.shape[1] + 2 * HALO
    padded = jnp.pad(visit_image, ((0, 2 * HALO), (0, 2 * HALO)))
    kernel_pad = jnp.pad(kernel, ((0, row_total - 2 * HALO), (0, col_total - 2 * HALO)))
    kernel_pad = jnp.roll(kernel_pad, (-HALO, -HALO), (0, 1))
    spectrum = jnp.fft.rfft2(padded) * jnp.fft.rfft2(kernel_pad)
    result = jnp.fft.irfft2(spectrum, s=(row_total, col_total))
    return result[:visit_image.shape[0], :visit_image.shape[1]].astype(visit_image.dtype)


def reference(piece_flux, piece_ivar, warp_rows, warp_cols, piece_owner, piece_slot, piece_extent, basis, coeffs):
    pieces = OWNERS * PIECES_DEV
    blocks = BR * BC

    def add_visit(totals, visit_data):
        flux_data, ivar_data, row_maps, col_maps, owner_idx, slot_idx, extent, weights = visit_data
        warped = warp_pieces(flux_data.reshape(pieces, S, S), ivar_data.reshape(pieces, S, S),
                             row_maps.reshape(pieces, S, S), col_maps.reshape(pieces, S, S),
                             extent.reshape(pieces, 2))
        target = owner_idx.reshape(pieces).astype(jnp.int32) * blocks + slot_idx.reshape(pieces).astype(jnp.int32)
        canvas = jnp.zeros((OWNERS * blocks, 2, S, S), warped.dtype).at[target].add(warped)
        canvas = canvas.reshape(OWNERS, BR, BC, 2, S, S).transpose(3, 0, 1, 4, 2, 5).reshape(2, NROWS, COLS)
        flux_sum = canvas[0]
        ivar_sum = canvas[1]
        visit_image = flux_sum / jnp.maximum(ivar_sum, 1.0)
        kernel = jnp.einsum("k,kij->ij", weights, basis, precision=HIGHEST_PREC)
        matched = match_psf(visit_image, kernel)
        return (totals[0] + ivar_sum * matched, totals[1] + ivar_sum), None

    empty = jnp.zeros((NROWS, COLS), piece_flux.dtype)
    sums, unused = lax.scan(add_visit, (empty, empty),
                            (piece_flux, piece_ivar, warp_rows, warp_cols, piece_owner, piece_slot, piece_extent, coeffs))
    numerator, weight_map = sums
    coadd = numerator / jnp.maximum(weight_map, 1.0)
    return coadd, weight_map
```

```python
import numpy as np

import jax
import jax.numpy as jnp
from jax import lax
from jax.experimental import pallas as pl
from jax.experimental.pallas import tpu as pltpu
from jax.sharding import PartitionSpec as P

MESH = pl.DeviceIdType.MESH
F32 = jnp.float32
BF16 = jnp.bfloat16

S = 128
HALO = 64
BR = 2
BC = 8
CAP = 2
VISITS = 8
OWNERS = 32
PIECES = 32
BLOCKS = BR * BC
SLOTS = OWNERS * CAP
LEN = 256
WIDE = (BC + 1) * S
TALL = BR * S + 2 * HALO
STRIDE = 11


def split_np(table):
    table = table.astype(np.float32)
    high = table.astype(jnp.bfloat16)
    low = (table - high.astype(np.float32)).astype(jnp.bfloat16)
    return high, low


def dft_tables():
    freq = (np.arange(LEN // 2) + 0.5) * (2.0 * np.pi / LEN)
    places = np.arange(LEN)
    taps = np.arange(-HALO, HALO)
    full = np.concatenate([np.cos(freq[:, None] * places), np.sin(freq[:, None] * places)])
    kern = np.concatenate([np.cos(freq[:, None] * taps), np.sin(freq[:, None] * taps)])
    mid = full[:, HALO : HALO + S] / (LEN // 2)
    return [
        part
        for table in (full, full.T, mid, mid.T, kern, kern.T)
        for part in split_np(np.ascontiguousarray(table))
    ]


def split(x):
    high = x.astype(BF16)
    return high, (x - high.astype(F32)).astype(BF16)


NN = (((1,), (0,)), ((), ()))
NT = (((1,), (1,)), ((), ()))


def dot3(a, b, dims=NN):
    def one(p, q):
        return lax.dot_general(p, q, dims, preferred_element_type=F32)

    return one(a[0], b[0]) + (one(a[0], b[1]) + one(a[1], b[0]))


def kernel(
    tab_ref, coef_ref, flux_hbm, ivar_hbm, rows_hbm, cols_hbm, ids_ref, basis_ref,
    full_h, full_l, fullt_h, fullt_l, mid_h, mid_l, midt_h, midt_l,
    kern_h, kern_l, kernt_h, kernt_l,
    coadd_ref, weight_ref,
    flux_v, ivar_v, rows_v, cols_v, send, recv, ids_recv, canvas, image,
    vh, vl, fxh, fxl, spec, numer, own_out, land,
    in_sem, ids_send_sem, ids_recv_sem, send_sem, recv_sem, chain_send, chain_recv, halo_send, halo_recv,
):
    v = lax.axis_index("visit")
    b = lax.axis_index("bulk")
    x, y, c = b // 8, (b // 2) % 4, b % 2

    def device_at(step, sign):
        dx, dy, dc = step // 8, (step // 2) % 4, step % 2
        if sign < 0:
            dx, dy = 4 - dx, 4 - dy
        return ((x + dx) % 4 * 4 + (y + dy) % 4) * 2 + (c + dc) % 2

    right, left = (v + 1) % VISITS, (v + VISITS - 1) % VISITS

    loads = [
        pltpu.make_async_copy(src, dst, in_sem.at[k])
        for k, (src, dst) in enumerate(
            ((flux_hbm, flux_v), (ivar_hbm, ivar_v), (rows_hbm, rows_v), (cols_hbm, cols_v))
        )
    ]
    for load in loads:
        load.start()
    barrier = pltpu.get_barrier_semaphore()

    def greet(i, carry):
        pl.semaphore_signal(barrier, inc=1, device_id=(v, device_at(i, 1)), device_id_type=MESH)
        return carry

    lax.fori_loop(1, OWNERS, greet, 0)
    for z in (right, left):
        pl.semaphore_signal(barrier, inc=1, device_id=(z, b), device_id_type=MESH)

    def clear(i, carry):
        canvas[0, i] = jnp.zeros((S, S), F32)
        canvas[1, i] = jnp.zeros((S, S), F32)
        return carry

    lax.fori_loop(0, BLOCKS, clear, 0)

    @pl.when(b == 0)
    def _():
        image[0:HALO, :] = jnp.zeros((HALO, WIDE), F32)

    @pl.when(b == OWNERS - 1)
    def _():
        image[HALO + BR * S : TALL, :] = jnp.zeros((HALO, WIDE), F32)

    for load in loads:
        load.wait()
    pl.semaphore_wait(barrier, OWNERS - 1 + 2)

    def id_copy(i):
        to = device_at(i, 1)
        return pltpu.make_async_remote_copy(
            src_ref=ids_ref.at[to], dst_ref=ids_recv.at[i], send_sem=ids_send_sem.at[i],
            recv_sem=ids_recv_sem.at[i], device_id=(v, to), device_id_type=MESH)

    def plane_copy(plane, i):
        return pltpu.make_async_remote_copy(
            src_ref=send.at[plane, i], dst_ref=recv.at[plane, i], send_sem=send_sem.at[plane, i],
            recv_sem=recv_sem.at[plane, i], device_id=(v, device_at(i, 1)), device_id_type=MESH)

    row_at = lax.broadcasted_iota(jnp.int32, (S, S), 0)
    col_at = lax.broadcasted_iota(jnp.int32, (S, S), 1)

    def warp_slot(i, r):
        slot = device_at(i, 1) * CAP + r
        piece = tab_ref[slot]
        ok = (row_at < tab_ref[SLOTS + slot]) & (col_at < tab_ref[2 * SLOTS + slot])
        weighted = jnp.where(ok, ivar_v[piece], 0.0)
        both = jnp.concatenate([weighted * flux_v[piece], weighted], axis=1)
        half = dot3(split(rows_v[piece]), split(both))
        tall = jnp.concatenate([half[:, :S], half[:, S:]], axis=0)
        warped = dot3(split(tall), split(cols_v[piece]), NT)
        send[0, i, r] = warped[:S]
        send[1, i, r] = warped[S:]

    def warp_step(k, carry):
        i = (k * STRIDE) % OWNERS
        for r in range(CAP):
            warp_slot(i, r)

        id_copy(i).start()
        plane_copy(1, i).start()
        return carry

    lax.fori_loop(1, OWNERS, warp_step, 0)

    def flux_step(k, carry):
        plane_copy(0, (k * STRIDE) % OWNERS).start()
        return carry

    lax.fori_loop(1, OWNERS, flux_step, 0)
    for r in range(CAP):
        warp_slot(0, r)

    taps = coef_ref[0] * basis_ref[0]
    for k in range(1, 4):
        taps = taps + coef_ref[k] * basis_ref[k]
    half_spec = dot3((kern_h[...], kern_l[...]), split(taps))
    spec[...] = dot3(split(half_spec), (kernt_h[...], kernt_l[...]))

    def add_slots(plane, id_rows, source, i):
        for r in range(CAP):
            pass
        first = jnp.broadcast_to(id_rows[0:1, :], (8, S))
        second = jnp.broadcast_to(id_rows[1:2, :], (8, S))

        def rows_step(q, carry):
            at = pl.ds(pl.multiple_of(q * 8, 8), 8)
            one = source[plane, i, 0, at, :]
            two = source[plane, i, 1, at, :]
            for block in range(BLOCKS):
                canvas[plane, block, at, :] = canvas[plane, block, at, :] + (
                    jnp.where(first == float(block), one, 0.0)
                    + jnp.where(second == float(block), two, 0.0))
            return carry

        lax.fori_loop(0, S // 8, rows_step, 0)

    add_slots(1, ids_ref[b], send, 0)

    def ivar_in(k, carry):
        i = (k * STRIDE) % OWNERS
        id_copy(i).wait_recv()
        plane_copy(1, i).wait_recv()
        add_slots(1, ids_recv[i], recv, i)
        return carry

    lax.fori_loop(1, OWNERS, ivar_in, 0)

    def chunk_of(direction, step):
        return (v + 4 - step) % VISITS if direction == 0 else (v + 4 + step) % VISITS

    def chain_copy(what, direction, step, half):
        return pltpu.make_async_remote_copy(
            src_ref=own_out.at[what, direction, step, half], dst_ref=land.at[what, direction, step, half],
            send_sem=chain_send.at[what, direction, step, half],
            recv_sem=chain_recv.at[what, direction, step, half],
            device_id=(right if direction == 0 else left, b), device_id_type=MESH)

    def chain_first(what, own):
        for direction in (0, 1):
            own_out[what, direction, 0, direction] = own(direction, chunk_of(direction, 0))
            chain_copy(what, direction, 0, direction).start()

    def chain_step(what, step, own):
        for near in (0, 1):
            for direction in (0, 1):
                half = direction if near == 0 else 1 - direction
                value = own(half, chunk_of(direction, step))
                if step > 1 or half == direction:
                    chain_copy(what, direction, step - 1, half).wait_recv()
                    value = value + land[what, direction, step - 1, half]
                own_out[what, direction, step, half] = value
                chain_copy(what, direction, step, half).start()

    def chain_last(what, half, own):
        for direction in (0, 1):
            chain_copy(what, direction, 3, half).wait_recv()
        return own(half, v) + (land[what, 0, 3, half] + land[what, 1, 3, half])

    def ivar_own(half, chunk):
        return canvas[1, half * BC + chunk]

    chain_first(1, ivar_own)
    add_slots(0, ids_ref[b], send, 0)

    def flux_in(k, carry):
        i = (k * STRIDE) % OWNERS
        plane_copy(0, i).wait_recv()
        add_slots(0, ids_recv[i], recv, i)
        return carry

    lax.fori_loop(1, 8, flux_in, 0)
    chain_step(1, 1, ivar_own)
    lax.fori_loop(8, 16, flux_in, 0)
    chain_step(1, 2, ivar_own)
    lax.fori_loop(16, 23, flux_in, 0)
    chain_step(1, 3, ivar_own)
    lax.fori_loop(23, 30, flux_in, 0)
    for half in range(BR):
        weight_ref[half * S : half * S + S, :] = chain_last(1, half, ivar_own)
    lax.fori_loop(30, OWNERS, flux_in, 0)

    for br in range(BR):
        before = jnp.zeros((S, HALO), F32)
        for j in range(BC + 1):
            if j < BC:
                cur = canvas[0, br * BC + j] / jnp.maximum(canvas[1, br * BC + j], 1.0)
                piece = jnp.concatenate([before, cur[:, :HALO]], axis=1)
                before = cur[:, HALO:]
            else:
                piece = jnp.concatenate([before, jnp.zeros((S, HALO), F32)], axis=1)
            image[HALO + br * S : HALO + br * S + S, j * S : j * S + S] = piece

    def halo_copy(side):
        start, to = (BR * S, 0) if side == 0 else (HALO, HALO + BR * S)
        return pltpu.make_async_remote_copy(
            src_ref=image.at[start : start + HALO, :], dst_ref=image.at[to : to + HALO, :],
            send_sem=halo_send.at[side], recv_sem=halo_recv.at[side],
            device_id=(v, (b + 1) % OWNERS if side == 0 else (b + OWNERS - 1) % OWNERS),
            device_id_type=MESH)

    has_next, has_before = b < OWNERS - 1, b > 0

    @pl.when(has_next)
    def _():
        halo_copy(0).start()

    @pl.when(has_before)
    def _():
        halo_copy(1).start()

    mine = slice(HALO, HALO + BR * S)
    vh[mine, :], vl[mine, :] = split(image[mine, :])

    @pl.when(has_before)
    def _():
        halo_copy(0).wait_recv()

    @pl.when(has_next)
    def _():
        halo_copy(1).wait_recv()

    for top in (0, HALO + BR * S):
        edge = slice(top, top + HALO)
        vh[edge, :], vl[edge, :] = split(image[edge, :])

    def row_stage(j, carry):
        at = pl.ds(pl.multiple_of(j * S, S), S)
        for rt in range(BR):
            here = slice(rt * S, rt * S + LEN)
            out = dot3((full_h[...], full_l[...]), (vh[here, at], vl[here, at]))
            there = slice(rt * LEN, rt * LEN + LEN)
            fxh[there, at], fxl[there, at] = split(out)
        return carry

    lax.fori_loop(0, BC + 1, row_stage, 0)

    def tile(bc):
        at = pl.ds(pl.multiple_of(bc * S, S), LEN)
        kcc, kcs = spec[:S, :S], spec[:S, S:]
        ksc, kss = spec[S:, :S], spec[S:, S:]
        for rt in range(BR):
            there = slice(rt * LEN, rt * LEN + LEN)
            freq = dot3((fxh[there, at], fxl[there, at]), (fullt_h[...], fullt_l[...]))
            xcc, xcs = freq[:S, :S], freq[:S, S:]
            xsc, xss = freq[S:, :S], freq[S:, S:]
            ycc = (xcc * kcc - xcs * kcs) - (xsc * ksc - xss * kss)
            ycs = (xcc * kcs + xcs * kcc) - (xsc * kss + xss * ksc)
            ysc = (xcc * ksc - xcs * kss) + (xsc * kcc - xss * kcs)
            yss = (xcc * kss + xcs * ksc) + (xsc * kcs + xss * kcc)
            prod = jnp.concatenate(
                [jnp.concatenate([ycc, ycs], axis=1), jnp.concatenate([ysc, yss], axis=1)], axis=0)
            back = dot3(split(prod), (mid_h[...], mid_l[...]))
            matched = dot3((midt_h[...], midt_l[...]), split(back))
            numer[rt, bc] = canvas[1, rt * BC + bc] * matched

    def numer_own(half, chunk):
        return numer[half, chunk]

    def tile_step(k, carry):
        near = (k + 1) // 2
        tile((v + 4 + jnp.where(k % 2 == 0, near, VISITS - near)) % VISITS)

        @pl.when(k == 0)
        def _():
            chain_first(0, numer_own)

        for step in (1, 2, 3):
            @pl.when(k == 2 * step)
            def _(step=step):
                chain_step(0, step, numer_own)

        return carry

    lax.fori_loop(0, VISITS, tile_step, 0)
    for half in range(BR):
        at = slice(half * S, half * S + S)
        coadd_ref[at, :] = chain_last(0, half, numer_own) / jnp.maximum(weight_ref[at, :], 1.0)

    def drain(i, carry):
        id_copy(i).wait_send()
        plane_copy(0, i).wait_send()
        plane_copy(1, i).wait_send()
        return carry

    lax.fori_loop(1, OWNERS, drain, 0)
    for what in (0, 1):
        for direction in (0, 1):
            chain_copy(what, direction, 0, direction).wait_send()
            for step in (1, 2, 3):
                for half in (0, 1):
                    chain_copy(what, direction, step, half).wait_send()

    @pl.when(has_next)
    def _():
        halo_copy(0).wait_send()

    @pl.when(has_before)
    def _():
        halo_copy(1).wait_send()


def on_device(piece_flux, piece_ivar, warp_rows, warp_cols, piece_owner, piece_slot, piece_extent, basis, coeffs):
    owner = piece_owner.reshape(PIECES)
    slot_id = piece_slot.reshape(PIECES)
    extent = piece_extent.reshape(PIECES, 2)
    order = jnp.arange(PIECES, dtype=jnp.int32)
    earlier = (owner[:, None] == owner[None, :]) & (order[None, :] < order[:, None])
    dest = owner * CAP + jnp.sum(earlier.astype(jnp.int32), axis=1)
    hit = dest[:, None] == jnp.arange(SLOTS, dtype=jnp.int32)[None, :]
    facts = jnp.stack([order, extent[:, 0], extent[:, 1], slot_id + 1])
    table = jnp.sum(jnp.where(hit[None], facts[:, :, None], 0), axis=1)
    ids = (table[3] - 1).astype(F32).reshape(OWNERS, CAP, 1)
    ids = jnp.broadcast_to(ids, (OWNERS, CAP, S))
    shape = (PIECES, S, S)
    vmem = pl.BlockSpec(memory_space=pltpu.VMEM)
    smem = pl.BlockSpec(memory_space=pltpu.SMEM)
    hbm = pl.BlockSpec(memory_space=pl.ANY)
    tables = dft_tables()
    dma = pltpu.SemaphoreType.DMA
    coadd, weight = pl.pallas_call(
        kernel,
        out_shape=[jax.ShapeDtypeStruct((BR * S, S), F32)] * 2,
        in_specs=[smem, smem, hbm, hbm, hbm, hbm] + [vmem] * (2 + len(tables)),
        out_specs=[vmem, vmem],
        scratch_shapes=[pltpu.VMEM(shape, F32)] * 4
        + [
            pltpu.VMEM((2, OWNERS, CAP, S, S), F32),
            pltpu.VMEM((2, OWNERS, CAP, S, S), F32),
            pltpu.VMEM((OWNERS, CAP, S), F32),
            pltpu.VMEM((2, BLOCKS, S, S), F32),
            pltpu.VMEM((TALL, WIDE), F32),
            pltpu.VMEM((TALL, WIDE), BF16),
            pltpu.VMEM((TALL, WIDE), BF16),
            pltpu.VMEM((BR * LEN, WIDE), BF16),
            pltpu.VMEM((BR * LEN, WIDE), BF16),
            pltpu.VMEM((LEN, LEN), F32),
            pltpu.VMEM((BR, BC, S, S), F32),
            pltpu.VMEM((2, 2, 4, 2, S, S), F32),
            pltpu.VMEM((2, 2, 4, 2, S, S), F32),
            dma((4,)),
            dma((OWNERS,)),
            dma((OWNERS,)),
            dma((2, OWNERS)),
            dma((2, OWNERS)),
            dma((2, 2, 4, 2)),
            dma((2, 2, 4, 2)),
            dma((2,)),
            dma((2,)),
        ],
        compiler_params=pltpu.CompilerParams(
            collective_id=0, has_side_effects=True, vmem_limit_bytes=60 * 1024 * 1024
        ),
        name="coadd",
    )(
        table[:3].reshape(3 * SLOTS), coeffs.reshape(4),
        piece_flux.reshape(shape), piece_ivar.reshape(shape), warp_rows.reshape(shape), warp_cols.reshape(shape),
        ids, basis, *[jnp.asarray(t) for t in tables],
    )
    return coadd, weight


def solution(mesh):
    piece = P("visit", "bulk", None, None, None)
    return jax.shard_map(
        on_device,
        mesh=mesh,
        in_specs=(piece, piece, piece, piece, P("visit", "bulk", None, None), P("visit", "bulk", None),
                  P("visit", "bulk", None, None), P(), P("visit", None)),
        out_specs=(P("bulk", "visit"), P("bulk", "visit")),
        check_vma=False,
    )
```

```python
import numpy as np

import jax
import jax.numpy as jnp
from jax import lax
from jax.experimental import pallas as pl
from jax.experimental.pallas import tpu as pltpu
from jax.sharding import PartitionSpec as P

MESH = pl.DeviceIdType.MESH
F32 = jnp.float32
BF16 = jnp.bfloat16

S = 128
HALO = 64
BR = 2
BC = 8
CAP = 2
VISITS = 8
OWNERS = 32
PIECES = 32
BLOCKS = BR * BC
PART = S // 2
LEN = 256
WIDE = (BC + 1) * S
TALL = BR * S + 2 * HALO
STRIDE = 11


def split_np(table):
    table = table.astype(np.float32)
    high = table.astype(jnp.bfloat16)
    low = (table - high.astype(np.float32)).astype(jnp.bfloat16)
    return high, low


def dft_tables():
    freq = (np.arange(LEN // 2) + 0.5) * (2.0 * np.pi / LEN)
    places = np.arange(LEN)
    taps = np.arange(-HALO, HALO)
    full = np.concatenate([np.cos(freq[:, None] * places), np.sin(freq[:, None] * places)])
    kern = np.concatenate([np.cos(freq[:, None] * taps), np.sin(freq[:, None] * taps)])
    mid = full[:, HALO : HALO + S] / (LEN // 2)
    return [
        part
        for table in (full, full.T, mid, mid.T, kern, kern.T)
        for part in split_np(np.ascontiguousarray(table))
    ]


def split(x):
    high = x.astype(BF16)
    return high, (x - high.astype(F32)).astype(BF16)


NN = (((1,), (0,)), ((), ()))
NT = (((1,), (1,)), ((), ()))


def dot3(a, b, dims=NN):
    def one(p, q):
        return lax.dot_general(p, q, dims, preferred_element_type=F32)

    return one(a[0], b[0]) + (one(a[0], b[1]) + one(a[1], b[0]))


def kernel(
    first_ref, last_ref, slot_ref, extent_ref, coef_ref, flux_hbm, ivar_hbm, rows_hbm, cols_hbm, basis_ref,
    full_h, full_l, fullt_h, fullt_l, mid_h, mid_l, midt_h, midt_l,
    kern_h, kern_l, kernt_h, kernt_l,
    coadd_ref, weight_ref,
    flux_v, ivar_v, rows_v, cols_v, send, recv, ids_own, ids_recv, dense, passed, arrived, canvas, image,
    vh, vl, fxh, fxl, spec, numer, own_out, land,
    in_sem, ids_send_sem, ids_recv_sem, send_sem, recv_sem, pass_send, pass_recv,
    chain_send, chain_recv, halo_send, halo_recv,
):
    v = lax.axis_index("visit")
    b = lax.axis_index("bulk")
    x, y, c = b // 8, (b // 2) % 4, b % 2

    def device_at(dx, dy, dc):
        return ((x + dx) % 4 * 4 + (y + dy) % 4) * 2 + (c + dc) % 2

    right, left = (v + 1) % VISITS, (v + VISITS - 1) % VISITS

    loads = [
        pltpu.make_async_copy(src, dst, in_sem.at[k])
        for k, (src, dst) in enumerate(
            ((flux_hbm, flux_v), (ivar_hbm, ivar_v), (rows_hbm, rows_v), (cols_hbm, cols_v))
        )
    ]
    for load in loads:
        load.start()
    barrier = pltpu.get_barrier_semaphore()

    def greet(i, carry):
        pl.semaphore_signal(barrier, inc=1, device_id=(v, (b + i) % OWNERS), device_id_type=MESH)
        return carry

    lax.fori_loop(1, OWNERS, greet, 0)
    for z in (right, left):
        pl.semaphore_signal(barrier, inc=1, device_id=(z, b), device_id_type=MESH)

    def line_device(route, j):
        return jnp.where(route == 0, device_at(j // 2, 0, j % 2), device_at(0, j // 2, j % 2))

    def owner_at(route, j, e):
        return jnp.where(route == 0, device_at(j // 2, e, j % 2), device_at(e, j // 2, j % 2))

    tile_row = lax.broadcasted_iota(jnp.int32, (8, S), 0)

    def make_ids(n, carry):
        route, j = n // 8, n % 8
        rows = jnp.zeros((8, S), F32)
        for e in range(4):
            owner = owner_at(route, j, e)
            low, high = first_ref[owner], last_ref[owner]
            one = jnp.where(high >= 0, slot_ref[jnp.minimum(low, PIECES - 1)], -1)
            two = jnp.where(high > low, slot_ref[jnp.maximum(high, 0)], -1)
            rows = jnp.where(tile_row == 2 * e, one.astype(F32), rows)
            rows = jnp.where(tile_row == 2 * e + 1, two.astype(F32), rows)
        ids_own[route, j] = rows
        return carry

    lax.fori_loop(0, 16, make_ids, 0)

    @pl.when(b == 0)
    def _():
        image[0:HALO, :] = jnp.zeros((HALO, WIDE), F32)

    @pl.when(b == OWNERS - 1)
    def _():
        image[HALO + BR * S : TALL, :] = jnp.zeros((HALO, WIDE), F32)

    for load in loads:
        load.wait()
    pl.semaphore_wait(barrier, OWNERS - 1 + 2)

    def id_copy(route, j):
        return pltpu.make_async_remote_copy(
            src_ref=ids_own.at[route, j], dst_ref=ids_recv.at[route, j], send_sem=ids_send_sem.at[route, j],
            recv_sem=ids_recv_sem.at[route, j], device_id=(v, line_device(route, j)), device_id_type=MESH)

    def part_copy(plane, route, j, e):
        return pltpu.make_async_remote_copy(
            src_ref=send.at[plane, route, j, e], dst_ref=recv.at[plane, route, j, e],
            send_sem=send_sem.at[plane, route, j], recv_sem=recv_sem.at[plane, route, j],
            device_id=(v, line_device(route, j)), device_id_type=MESH)

    def line_copy(plane, route, j):
        return pltpu.make_async_remote_copy(
            src_ref=send.at[plane, route, j], dst_ref=recv.at[plane, route, j],
            send_sem=send_sem.at[plane, route, j], recv_sem=recv_sem.at[plane, route, j],
            device_id=(v, line_device(route, j)), device_id_type=MESH)

    def send_ids(n, carry):
        id_copy(n % 2, n // 2).start()
        return carry

    lax.fori_loop(2, 16, send_ids, 0)

    row_at = lax.broadcasted_iota(jnp.int32, (S, S), 0)
    col_at = lax.broadcasted_iota(jnp.int32, (S, S), 1)

    def warp_slot(i, r):
        dx, dy, dc = i // 8, (i // 2) % 4, i % 2
        owner = device_at(dx, dy, dc)
        piece = jnp.minimum(first_ref[owner], PIECES - 1) if r == 0 else jnp.maximum(last_ref[owner], 0)
        ok = (row_at < extent_ref[0, piece]) & (col_at < extent_ref[1, piece])
        weighted = jnp.where(ok, ivar_v[piece], 0.0)
        both = jnp.concatenate([weighted * flux_v[piece], weighted], axis=1)
        half = dot3(split(rows_v[piece]), split(both))
        tall = jnp.concatenate([half[:, :S], half[:, S:]], axis=0)
        warped = dot3(split(tall), split(cols_v[piece]), NT)
        for plane in (0, 1):
            send[plane, 0, dx * 2 + dc, dy, r] = warped[plane * S : plane * S + PART]
            send[plane, 1, dy * 2 + dc, dx, r] = warped[plane * S + PART : plane * S + S]

    def send_parts(plane, i):
        dx, dy, dc = i // 8, (i // 2) % 4, i % 2

        @pl.when(dx + dc > 0)
        def _():
            part_copy(plane, 0, dx * 2 + dc, dy).start()

        @pl.when(dy + dc > 0)
        def _():
            part_copy(plane, 1, dy * 2 + dc, dx).start()

    def warp_step(k, carry):
        i = (k * STRIDE) % OWNERS
        for r in range(CAP):
            warp_slot(i, r)
        send_parts(1, i)
        return carry

    lax.fori_loop(1, OWNERS, warp_step, 0)

    def flux_step(k, carry):
        send_parts(0, (k * STRIDE) % OWNERS)
        return carry

    lax.fori_loop(1, OWNERS, flux_step, 0)
    for r in range(CAP):
        warp_slot(0, r)

    taps = coef_ref[0] * basis_ref[0]
    for k in range(1, 4):
        taps = taps + coef_ref[k] * basis_ref[k]
    half_spec = dot3((kern_h[...], kern_l[...]), split(taps))
    spec[...] = dot3(split(half_spec), (kernt_h[...], kernt_l[...]))

    def add_line(plane, route, j, source, ids, fresh):
        marks = ids[route, j]

        def rows_step(q, carry):
            at = pl.ds(pl.multiple_of(q * 8, 8), 8)
            for e in range(4):
                first = jnp.broadcast_to(marks[2 * e : 2 * e + 1, :], (8, S))
                second = jnp.broadcast_to(marks[2 * e + 1 : 2 * e + 2, :], (8, S))
                one = source[plane, route, j, e, 0, at, :]
                two = source[plane, route, j, e, 1, at, :]
                for block in range(BLOCKS):
                    value = jnp.where(first == float(block), one, 0.0) + jnp.where(second == float(block), two, 0.0)
                    if not fresh:
                        value = dense[plane, route, e, block, at, :] + value
                    dense[plane, route, e, block, at, :] = value
            return carry

        lax.fori_loop(0, PART // 8, rows_step, 0)

    def add_plane(plane):
        def own(n, carry):
            add_line(plane, n, 0, send, ids_own, True)
            return carry

        def landed(n, carry):
            route, j = n % 2, n // 2
            line_copy(plane, route, j).wait_recv()
            add_line(plane, route, j, recv, ids_recv, False)
            return carry

        lax.fori_loop(0, 2, own, 0)
        lax.fori_loop(2, 16, landed, 0)

    LOW, HIGH = slice(0, BLOCKS // 2), slice(BLOCKS // 2, BLOCKS)

    def pass_copy(plane, route, m):
        ahead = m % 2 == 0
        step = 1 if ahead else 3
        to = device_at(0, step, 0) if route == 0 else device_at(step, 0, 0)
        way = 0 if ahead else 1
        if m < 2:
            src = dense.at[plane, route, 2, LOW if ahead else HIGH]
            dst = passed.at[plane, route, way]
        else:
            part = (HIGH if ahead else LOW) if m < 4 else (LOW if ahead else HIGH)
            src = dense.at[plane, route, step, part]
            dst = arrived.at[plane, route, way, part]
        return pltpu.make_async_remote_copy(
            src_ref=src, dst_ref=dst, send_sem=pass_send.at[plane, route, m], recv_sem=pass_recv.at[plane, route, m],
            device_id=(v, to), device_id_type=MESH)

    def pass_first(plane):
        for m in range(4):
            for route in (0, 1):
                pass_copy(plane, route, m).start()

    def pass_merged(plane):
        for m in (4, 5):
            for route in (0, 1):
                pass_copy(plane, route, m - 4).wait_recv()

                def merge(block, carry, m=m, route=route):
                    there = block if m == 4 else block + BLOCKS // 2
                    step = 1 if m == 4 else 3
                    dense[plane, route, step, there] = dense[plane, route, step, there] + passed[plane, route, m - 4, block]
                    return carry

                lax.fori_loop(0, BLOCKS // 2, merge, 0)
                pass_copy(plane, route, m).start()

    def pass_last(plane):
        for route in (0, 1):
            for m in (2, 3, 4, 5):
                pass_copy(plane, route, m).wait_recv()
            rows = slice(route * PART, route * PART + PART)

            def total(block, carry, route=route, rows=rows):
                canvas[plane, block, rows, :] = dense[plane, route, 0, block] + (
                    arrived[plane, route, 0, block] + arrived[plane, route, 1, block])
                return carry

            lax.fori_loop(0, BLOCKS, total, 0)

    def ids_in(n, carry):
        id_copy(n % 2, n // 2).wait_recv()
        return carry

    lax.fori_loop(2, 16, ids_in, 0)
    add_plane(1)
    pass_first(1)
    add_plane(0)
    pass_merged(1)
    pass_first(0)
    pass_last(1)

    def chunk_of(direction, step):
        return (v + 4 - step) % VISITS if direction == 0 else (v + 4 + step) % VISITS

    def chain_copy(what, direction, step, half):
        return pltpu.make_async_remote_copy(
            src_ref=own_out.at[what, direction, step, half], dst_ref=land.at[what, direction, step, half],
            send_sem=chain_send.at[what, direction, step, half],
            recv_sem=chain_recv.at[what, direction, step, half],
            device_id=(right if direction == 0 else left, b), device_id_type=MESH)

    def chain_first(what, own):
        for direction in (0, 1):
            own_out[what, direction, 0, direction] = own(direction, chunk_of(direction, 0))
            chain_copy(what, direction, 0, direction).start()

    def chain_step(what, step, own):
        for near in (0, 1):
            for direction in (0, 1):
                half = direction if near == 0 else 1 - direction
                value = own(half, chunk_of(direction, step))
                if step > 1 or half == direction:
                    chain_copy(what, direction, step - 1, half).wait_recv()
                    value = value + land[what, direction, step - 1, half]
                own_out[what, direction, step, half] = value
                chain_copy(what, direction, step, half).start()

    def chain_last(what, half, own):
        for direction in (0, 1):
            chain_copy(what, direction, 3, half).wait_recv()
        return own(half, v) + (land[what, 0, 3, half] + land[what, 1, 3, half])

    def ivar_own(half, chunk):
        return canvas[1, half * BC + chunk]

    chain_first(1, ivar_own)
    pass_merged(0)
    for step in (1, 2, 3):
        chain_step(1, step, ivar_own)
    pass_last(0)

    for br in range(BR):
        before = jnp.zeros((S, HALO), F32)
        for j in range(BC + 1):
            if j < BC:
                cur = canvas[0, br * BC + j] / jnp.maximum(canvas[1, br * BC + j], 1.0)
                piece = jnp.concatenate([before, cur[:, :HALO]], axis=1)
                before = cur[:, HALO:]
            else:
                piece = jnp.concatenate([before, jnp.zeros((S, HALO), F32)], axis=1)
            image[HALO + br * S : HALO + br * S + S, j * S : j * S + S] = piece

    def halo_copy(side):
        start, to = (BR * S, 0) if side == 0 else (HALO, HALO + BR * S)
        return pltpu.make_async_remote_copy(
            src_ref=image.at[start : start + HALO, :], dst_ref=image.at[to : to + HALO, :],
            send_sem=halo_send.at[side], recv_sem=halo_recv.at[side],
            device_id=(v, (b + 1) % OWNERS if side == 0 else (b + OWNERS - 1) % OWNERS),
            device_id_type=MESH)

    has_next, has_before = b < OWNERS - 1, b > 0

    @pl.when(has_next)
    def _():
        halo_copy(0).start()

    @pl.when(has_before)
    def _():
        halo_copy(1).start()

    mine = slice(HALO, HALO + BR * S)
    vh[mine, :], vl[mine, :] = split(image[mine, :])
    for half in range(BR):
        weight_ref[half * S : half * S + S, :] = chain_last(1, half, ivar_own)

    @pl.when(has_before)
    def _():
        halo_copy(0).wait_recv()

    @pl.when(has_next)
    def _():
        halo_copy(1).wait_recv()

    for top in (0, HALO + BR * S):
        edge = slice(top, top + HALO)
        vh[edge, :], vl[edge, :] = split(image[edge, :])

    def row_stage(j, carry):
        at = pl.ds(pl.multiple_of(j * S, S), S)
        for rt in range(BR):
            here = slice(rt * S, rt * S + LEN)
            out = dot3((full_h[...], full_l[...]), (vh[here, at], vl[here, at]))
            there = slice(rt * LEN, rt * LEN + LEN)
            fxh[there, at], fxl[there, at] = split(out)
        return carry

    lax.fori_loop(0, BC + 1, row_stage, 0)

    def tile(bc):
        at = pl.ds(pl.multiple_of(bc * S, S), LEN)
        kcc, kcs = spec[:S, :S], spec[:S, S:]
        ksc, kss = spec[S:, :S], spec[S:, S:]
        for rt in range(BR):
            there = slice(rt * LEN, rt * LEN + LEN)
            freq = dot3((fxh[there, at], fxl[there, at]), (fullt_h[...], fullt_l[...]))
            xcc, xcs = freq[:S, :S], freq[:S, S:]
            xsc, xss = freq[S:, :S], freq[S:, S:]
            ycc = (xcc * kcc - xcs * kcs) - (xsc * ksc - xss * kss)
            ycs = (xcc * kcs + xcs * kcc) - (xsc * kss + xss * ksc)
            ysc = (xcc * ksc - xcs * kss) + (xsc * kcc - xss * kcs)
            yss = (xcc * kss + xcs * ksc) + (xsc * kcs + xss * kcc)
            prod = jnp.concatenate(
                [jnp.concatenate([ycc, ycs], axis=1), jnp.concatenate([ysc, yss], axis=1)], axis=0)
            back = dot3(split(prod), (mid_h[...], mid_l[...]))
            matched = dot3((midt_h[...], midt_l[...]), split(back))
            numer[rt, bc] = canvas[1, rt * BC + bc] * matched

    def numer_own(half, chunk):
        return numer[half, chunk]

    def tile_step(k, carry):
        near = (k + 1) // 2
        tile((v + 4 + jnp.where(k % 2 == 0, near, VISITS - near)) % VISITS)

        @pl.when(k == 0)
        def _():
            chain_first(0, numer_own)

        for step in (1, 2, 3):
            @pl.when(k == 2 * step)
            def _(step=step):
                chain_step(0, step, numer_own)

        return carry

    lax.fori_loop(0, VISITS, tile_step, 0)
    for half in range(BR):
        at = slice(half * S, half * S + S)
        coadd_ref[at, :] = chain_last(0, half, numer_own) / jnp.maximum(weight_ref[at, :], 1.0)

    def drain(n, carry):
        route, j = n % 2, n // 2
        id_copy(route, j).wait_send()
        line_copy(0, route, j).wait_send()
        line_copy(1, route, j).wait_send()
        return carry

    lax.fori_loop(2, 16, drain, 0)
    for plane in (0, 1):
        for route in (0, 1):
            for m in range(6):
                pass_copy(plane, route, m).wait_send()
    for what in (0, 1):
        for direction in (0, 1):
            chain_copy(what, direction, 0, direction).wait_send()
            for step in (1, 2, 3):
                for half in (0, 1):
                    chain_copy(what, direction, step, half).wait_send()

    @pl.when(has_next)
    def _():
        halo_copy(0).wait_send()

    @pl.when(has_before)
    def _():
        halo_copy(1).wait_send()


def on_device(piece_flux, piece_ivar, warp_rows, warp_cols, piece_owner, piece_slot, piece_extent, basis, coeffs):
    owner = piece_owner.reshape(PIECES)
    order = jnp.arange(PIECES, dtype=jnp.int32)
    hit = owner[:, None] == jnp.arange(OWNERS, dtype=jnp.int32)[None, :]
    first = jnp.min(jnp.where(hit, order[:, None], PIECES), axis=0)
    last = jnp.max(jnp.where(hit, order[:, None], -1), axis=0)
    shape = (PIECES, S, S)
    vmem = pl.BlockSpec(memory_space=pltpu.VMEM)
    smem = pl.BlockSpec(memory_space=pltpu.SMEM)
    hbm = pl.BlockSpec(memory_space=pl.ANY)
    tables = dft_tables()
    dma = pltpu.SemaphoreType.DMA
    coadd, weight = pl.pallas_call(
        kernel,
        out_shape=[jax.ShapeDtypeStruct((BR * S, S), F32)] * 2,
        in_specs=[smem] * 5 + [hbm] * 4 + [vmem] * (1 + len(tables)),
        out_specs=[vmem, vmem],
        scratch_shapes=[pltpu.VMEM(shape, F32)] * 4
        + [
            pltpu.VMEM((2, 2, 8, 4, CAP, PART, S), F32),
            pltpu.VMEM((2, 2, 8, 4, CAP, PART, S), F32),
            pltpu.VMEM((2, 8, 8, S), F32),
            pltpu.VMEM((2, 8, 8, S), F32),
            pltpu.VMEM((2, 2, 4, BLOCKS, PART, S), F32),
            pltpu.VMEM((2, 2, 2, BLOCKS // 2, PART, S), F32),
            pltpu.VMEM((2, 2, 2, BLOCKS, PART, S), F32),
            pltpu.VMEM((2, BLOCKS, S, S), F32),
            pltpu.VMEM((TALL, WIDE), F32),
            pltpu.VMEM((TALL, WIDE), BF16),
            pltpu.VMEM((TALL, WIDE), BF16),
            pltpu.VMEM((BR * LEN, WIDE), BF16),
            pltpu.VMEM((BR * LEN, WIDE), BF16),
            pltpu.VMEM((LEN, LEN), F32),
            pltpu.VMEM((BR, BC, S, S), F32),
            pltpu.VMEM((2, 2, 4, 2, S, S), F32),
            pltpu.VMEM((2, 2, 4, 2, S, S), F32),
            dma((4,)),
            dma((2, 8)),
            dma((2, 8)),
            dma((2, 2, 8)),
            dma((2, 2, 8)),
            dma((2, 2, 6)),
            dma((2, 2, 6)),
            dma((2, 2, 4, 2)),
            dma((2, 2, 4, 2)),
            dma((2,)),
            dma((2,)),
        ],
        compiler_params=pltpu.CompilerParams(
            collective_id=0, has_side_effects=True, vmem_limit_bytes=60 * 1024 * 1024
        ),
        name="coadd",
    )(
        first, last, piece_slot.reshape(PIECES), piece_extent.reshape(PIECES, 2).T, coeffs.reshape(4),
        piece_flux.reshape(shape), piece_ivar.reshape(shape), warp_rows.reshape(shape), warp_cols.reshape(shape),
        basis, *[jnp.asarray(t) for t in tables],
    )
    return coadd, weight


def solution(mesh):
    piece = P("visit", "bulk", None, None, None)
    return jax.shard_map(
        on_device,
        mesh=mesh,
        in_specs=(piece, piece, piece, piece, P("visit", "bulk", None, None), P("visit", "bulk", None),
                  P("visit", "bulk", None, None), P(), P("visit", None)),
        out_specs=(P("bulk", "visit"), P("bulk", "visit")),
        check_vma=False,
    )
```

```python
import numpy as np

import jax
import jax.numpy as jnp
from jax import lax
from jax.experimental import pallas as pl
from jax.experimental.pallas import tpu as pltpu
from jax.sharding import PartitionSpec as P

MESH = pl.DeviceIdType.MESH
F32 = jnp.float32
BF16 = jnp.bfloat16

S = 128
HALO = 64
BR = 2
BC = 8
CAP = 2
VISITS = 8
OWNERS = 32
PIECES = 32
BLOCKS = BR * BC
PART = S // 2
LEN = 256
WIDE = (BC + 1) * S
TALL = BR * S + 2 * HALO
STRIDE = 11
TABLES = 15
THIRD = WIDE // 3


def split_np(table):
    table = table.astype(np.float32)
    high = table.astype(jnp.bfloat16)
    low = (table - high.astype(np.float32)).astype(jnp.bfloat16)
    return high, low


def dft_tables():
    freq = (np.arange(LEN // 2) + 0.5) * (2.0 * np.pi / LEN)
    places = np.arange(LEN)
    taps = np.arange(-HALO, HALO)
    full = np.concatenate([np.cos(freq[:, None] * places), np.sin(freq[:, None] * places)])
    kern = np.concatenate([np.cos(freq[:, None] * taps), np.sin(freq[:, None] * taps)])
    mid = full[:, HALO : HALO + S] / (LEN // 2)
    parts = [
        part
        for table in (full, full.T, mid, mid.T, kern, kern.T)
        for part in split_np(np.ascontiguousarray(table))
    ]
    high, low = parts[:2]
    for cut in (slice(0, HALO), slice(LEN - HALO, LEN)):
        parts.append(np.concatenate([high[:, cut], high[:, cut], low[:, cut]], axis=1))
    return parts


def split(x):
    high = x.astype(BF16)
    return high, (x - high.astype(F32)).astype(BF16)


NN = (((1,), (0,)), ((), ()))
NT = (((1,), (1,)), ((), ()))


def dot3(a, b, dims=NN):
    def one(p, q):
        return lax.dot_general(p, q, dims, preferred_element_type=F32)

    return one(a[0], b[0]) + (one(a[0], b[1]) + one(a[1], b[0]))


def kernel(
    first_ref, last_ref, slot_ref, extent_ref, coef_ref, flux_hbm, ivar_hbm, rows_hbm, cols_hbm, *rest,
):
    tables_hbm, (coadd_ref, weight_ref) = rest[:TABLES], rest[TABLES : TABLES + 2]
    tables_v, scratch = rest[TABLES + 2 : 2 * TABLES + 2], rest[2 * TABLES + 2 :]
    (
        basis_ref, full_h, full_l, fullt_h, fullt_l, mid_h, mid_l, midt_h, midt_l,
        kern_h, kern_l, kernt_h, kernt_l, edge_first, edge_last,
    ) = tables_v
    (
    flux_v, ivar_v, rows_v, cols_v, send, recv, ids_own, ids_recv, dense, passed, arrived, canvas, image,
    vh, vl, fxh, fxl, spec, numer, own_out, land,
    in_sem, ids_send_sem, ids_recv_sem, send_sem, recv_sem, pass_send, pass_recv,
    chain_send, chain_recv, halo_send, halo_recv, table_sem, own_rows, edges,
    ) = scratch
    v = lax.axis_index("visit")
    b = lax.axis_index("bulk")
    x, y, c = b // 8, (b // 2) % 4, b % 2

    def device_at(dx, dy, dc):
        return ((x + dx) % 4 * 4 + (y + dy) % 4) * 2 + (c + dc) % 2

    right, left = (v + 1) % VISITS, (v + VISITS - 1) % VISITS

    pairs = ((flux_hbm, flux_v), (ivar_hbm, ivar_v), (rows_hbm, rows_v), (cols_hbm, cols_v))
    loads = [
        pltpu.make_async_copy(src.at[q * 8 : q * 8 + 8], dst.at[q * 8 : q * 8 + 8], in_sem.at[4 * k + q])
        for k, (src, dst) in enumerate(pairs)
        for q in range(4)
    ]
    table_loads = [
        pltpu.make_async_copy(src, dst, table_sem.at[k]) for k, (src, dst) in enumerate(zip(tables_hbm, tables_v))
    ]
    for load in loads:
        load.start()
    barrier = pltpu.get_barrier_semaphore()

    def greet(i, carry):
        pl.semaphore_signal(barrier, inc=1, device_id=(v, (b + i) % OWNERS), device_id_type=MESH)
        return carry

    lax.fori_loop(1, OWNERS, greet, 0)
    for z in (right, left):
        pl.semaphore_signal(barrier, inc=1, device_id=(z, b), device_id_type=MESH)

    def line_device(route, j):
        return jnp.where(route == 0, device_at(j // 2, 0, j % 2), device_at(0, j // 2, j % 2))

    def owner_at(route, j, e):
        return jnp.where(route == 0, device_at(j // 2, e, j % 2), device_at(e, j // 2, j % 2))

    tile_row = lax.broadcasted_iota(jnp.int32, (8, S), 0)

    def make_ids(n, carry):
        route, j = n // 8, n % 8
        rows = jnp.zeros((8, S), F32)
        for e in range(4):
            owner = owner_at(route, j, e)
            low, high = first_ref[owner], last_ref[owner]
            one = jnp.where(high >= 0, slot_ref[jnp.minimum(low, PIECES - 1)], -1)
            two = jnp.where(high > low, slot_ref[jnp.maximum(high, 0)], -1)
            rows = jnp.where(tile_row == 2 * e, one.astype(F32), rows)
            rows = jnp.where(tile_row == 2 * e + 1, two.astype(F32), rows)
        ids_own[route, j] = rows
        return carry

    lax.fori_loop(0, 16, make_ids, 0)

    @pl.when(b == 0)
    def _():
        image[0:HALO, :] = jnp.zeros((HALO, WIDE), F32)

    @pl.when(b == OWNERS - 1)
    def _():
        image[HALO + BR * S : TALL, :] = jnp.zeros((HALO, WIDE), F32)

    for load in loads:
        load.wait()
    for load in table_loads:
        load.start()
    pl.semaphore_wait(barrier, OWNERS - 1 + 2)

    def id_copy(route, j):
        return pltpu.make_async_remote_copy(
            src_ref=ids_own.at[route, j], dst_ref=ids_recv.at[route, j], send_sem=ids_send_sem.at[route, j],
            recv_sem=ids_recv_sem.at[route, j], device_id=(v, line_device(route, j)), device_id_type=MESH)

    def part_copy(plane, route, j, e):
        return pltpu.make_async_remote_copy(
            src_ref=send.at[plane, route, j, e], dst_ref=recv.at[plane, route, j, e],
            send_sem=send_sem.at[plane, route, j], recv_sem=recv_sem.at[plane, route, j],
            device_id=(v, line_device(route, j)), device_id_type=MESH)

    def line_copy(plane, route, j):
        return pltpu.make_async_remote_copy(
            src_ref=send.at[plane, route, j], dst_ref=recv.at[plane, route, j],
            send_sem=send_sem.at[plane, route, j], recv_sem=recv_sem.at[plane, route, j],
            device_id=(v, line_device(route, j)), device_id_type=MESH)

    def send_ids(n, carry):
        id_copy(n % 2, n // 2).start()
        return carry

    lax.fori_loop(2, 16, send_ids, 0)

    row_at = lax.broadcasted_iota(jnp.int32, (S, S), 0)
    col_at = lax.broadcasted_iota(jnp.int32, (S, S), 1)

    def warp_slot(i, r):
        dx, dy, dc = i // 8, (i // 2) % 4, i % 2
        owner = device_at(dx, dy, dc)
        piece = jnp.minimum(first_ref[owner], PIECES - 1) if r == 0 else jnp.maximum(last_ref[owner], 0)
        ok = (row_at < extent_ref[0, piece]) & (col_at < extent_ref[1, piece])
        weighted = jnp.where(ok, ivar_v[piece], 0.0)
        both = jnp.concatenate([weighted * flux_v[piece], weighted], axis=1)
        half = dot3(split(rows_v[piece]), split(both))
        tall = jnp.concatenate([half[:, :S], half[:, S:]], axis=0)
        warped = dot3(split(tall), split(cols_v[piece]), NT)
        for plane in (0, 1):
            send[plane, 0, dx * 2 + dc, dy, r] = warped[plane * S : plane * S + PART]
            send[plane, 1, dy * 2 + dc, dx, r] = warped[plane * S + PART : plane * S + S]

    def send_parts(plane, i):
        dx, dy, dc = i // 8, (i // 2) % 4, i % 2

        @pl.when(dx + dc > 0)
        def _():
            part_copy(plane, 0, dx * 2 + dc, dy).start()

        @pl.when(dy + dc > 0)
        def _():
            part_copy(plane, 1, dy * 2 + dc, dx).start()

    def warp_step(k, carry):
        i = (k * STRIDE) % OWNERS
        for r in range(CAP):
            warp_slot(i, r)
        send_parts(1, i)
        return carry

    lax.fori_loop(1, OWNERS, warp_step, 0)

    def flux_step(k, carry):
        send_parts(0, (k * STRIDE) % OWNERS)
        return carry

    lax.fori_loop(1, OWNERS, flux_step, 0)
    for r in range(CAP):
        warp_slot(0, r)

    for load in table_loads:
        load.wait()
    taps = coef_ref[0] * basis_ref[0]
    for k in range(1, 4):
        taps = taps + coef_ref[k] * basis_ref[k]
    half_spec = dot3((kern_h[...], kern_l[...]), split(taps))
    spec[...] = dot3(split(half_spec), (kernt_h[...], kernt_l[...]))

    def add_line(plane, route, j, source, ids, fresh):
        marks = ids[route, j]

        def rows_step(q, carry):
            at = pl.ds(pl.multiple_of(q * 8, 8), 8)
            for e in range(4):
                first = jnp.broadcast_to(marks[2 * e : 2 * e + 1, :], (8, S))
                second = jnp.broadcast_to(marks[2 * e + 1 : 2 * e + 2, :], (8, S))
                one = source[plane, route, j, e, 0, at, :]
                two = source[plane, route, j, e, 1, at, :]
                for block in range(BLOCKS):
                    value = jnp.where(first == float(block), one, 0.0) + jnp.where(second == float(block), two, 0.0)
                    if not fresh:
                        value = dense[plane, route, e, block, at, :] + value
                    dense[plane, route, e, block, at, :] = value
            return carry

        lax.fori_loop(0, PART // 8, rows_step, 0)

    def add_plane(plane):
        def own(n, carry):
            add_line(plane, n, 0, send, ids_own, True)
            return carry

        def landed(n, carry):
            route, j = n % 2, n // 2
            line_copy(plane, route, j).wait_recv()
            add_line(plane, route, j, recv, ids_recv, False)
            return carry

        lax.fori_loop(0, 2, own, 0)
        lax.fori_loop(2, 16, landed, 0)

    LOW, HIGH = slice(0, BLOCKS // 2), slice(BLOCKS // 2, BLOCKS)

    def pass_copy(plane, route, m):
        ahead = m % 2 == 0
        step = 1 if ahead else 3
        to = device_at(0, step, 0) if route == 0 else device_at(step, 0, 0)
        way = 0 if ahead else 1
        if m < 2:
            src = dense.at[plane, route, 2, LOW if ahead else HIGH]
            dst = passed.at[plane, route, way]
        else:
            part = (HIGH if ahead else LOW) if m < 4 else (LOW if ahead else HIGH)
            src = dense.at[plane, route, step, part]
            dst = arrived.at[plane, route, way, part]
        return pltpu.make_async_remote_copy(
            src_ref=src, dst_ref=dst, send_sem=pass_send.at[plane, route, m], recv_sem=pass_recv.at[plane, route, m],
            device_id=(v, to), device_id_type=MESH)

    def pass_first(plane):
        for m in range(4):
            for route in (0, 1):
                pass_copy(plane, route, m).start()

    def pass_merged(plane):
        for m in (4, 5):
            for route in (0, 1):
                pass_copy(plane, route, m - 4).wait_recv()

                def merge(block, carry, m=m, route=route):
                    there = block if m == 4 else block + BLOCKS // 2
                    step = 1 if m == 4 else 3
                    dense[plane, route, step, there] = dense[plane, route, step, there] + passed[plane, route, m - 4, block]
                    return carry

                lax.fori_loop(0, BLOCKS // 2, merge, 0)
                pass_copy(plane, route, m).start()

    def pass_last(plane):
        for route in (0, 1):
            for m in (2, 3, 4, 5):
                pass_copy(plane, route, m).wait_recv()
            rows = slice(route * PART, route * PART + PART)

            def total(block, carry, route=route, rows=rows):
                canvas[plane, block, rows, :] = dense[plane, route, 0, block] + (
                    arrived[plane, route, 0, block] + arrived[plane, route, 1, block])
                return carry

            lax.fori_loop(0, BLOCKS, total, 0)

    def ids_in(n, carry):
        id_copy(n % 2, n // 2).wait_recv()
        return carry

    lax.fori_loop(2, 16, ids_in, 0)
    add_plane(1)
    pass_first(1)
    add_plane(0)
    pass_merged(1)
    pass_first(0)
    pass_last(1)

    def chunk_of(direction, step):
        return (v + 4 - step) % VISITS if direction == 0 else (v + 4 + step) % VISITS

    def chain_copy(what, direction, step, quarter):
        return pltpu.make_async_remote_copy(
            src_ref=own_out.at[what, direction, step, quarter], dst_ref=land.at[what, direction, step, quarter],
            send_sem=chain_send.at[what, direction, step, quarter],
            recv_sem=chain_recv.at[what, direction, step, quarter],
            device_id=(right if direction == 0 else left, b), device_id_type=MESH)

    def chain_first(what, own):
        for near in (0, 1):
            for direction in (0, 1):
                quarter = 2 * direction + near
                own_out[what, direction, 0, quarter] = own(quarter, chunk_of(direction, 0))
                chain_copy(what, direction, 0, quarter).start()

    def chain_step(what, step, own):
        for near in range(4):
            for direction in (0, 1):
                quarter = (2 * direction + near) % 4
                value = own(quarter, chunk_of(direction, step))
                if step > 1 or near < 2:
                    chain_copy(what, direction, step - 1, quarter).wait_recv()
                    value = value + land[what, direction, step - 1, quarter]
                own_out[what, direction, step, quarter] = value
                chain_copy(what, direction, step, quarter).start()

    def chain_last(what, quarter, own):
        for direction in (0, 1):
            chain_copy(what, direction, 3, quarter).wait_recv()
        return own(quarter, v) + (land[what, 0, 3, quarter] + land[what, 1, 3, quarter])

    def ivar_own(quarter, chunk):
        return canvas[1, quarter // 2 * BC + chunk, quarter % 2 * PART : quarter % 2 * PART + PART, :]

    chain_first(1, ivar_own)
    pass_merged(0)
    for step in (1, 2):
        chain_step(1, step, ivar_own)
    pass_last(0)

    def make_image(br, start):
        rows = slice(start, start + PART)
        there = HALO + br * S + start
        before = jnp.zeros((PART, HALO), F32)
        for j in range(BC + 1):
            if j < BC:
                cur = canvas[0, br * BC + j, rows, :] / jnp.maximum(canvas[1, br * BC + j, rows, :], 1.0)
                piece = jnp.concatenate([before, cur[:, :HALO]], axis=1)
                before = cur[:, HALO:]
            else:
                piece = jnp.concatenate([before, jnp.zeros((PART, HALO), F32)], axis=1)
            image[there : there + PART, j * S : j * S + S] = piece

    def halo_copy(side):
        start, to = (BR * S, 0) if side == 0 else (HALO, HALO + BR * S)
        return pltpu.make_async_remote_copy(
            src_ref=image.at[start : start + HALO, :], dst_ref=image.at[to : to + HALO, :],
            send_sem=halo_send.at[side], recv_sem=halo_recv.at[side],
            device_id=(v, (b + 1) % OWNERS if side == 0 else (b + OWNERS - 1) % OWNERS),
            device_id_type=MESH)

    has_next, has_before = b < OWNERS - 1, b > 0

    make_image(1, PART)

    @pl.when(has_next)
    def _():
        halo_copy(0).start()

    make_image(0, 0)

    @pl.when(has_before)
    def _():
        halo_copy(1).start()

    make_image(0, PART)
    make_image(1, 0)
    mine = slice(HALO, HALO + BR * S)
    vh[mine, :], vl[mine, :] = split(image[mine, :])
    for top in (0, HALO + BR * S):
        vh[top : top + HALO, :] = jnp.zeros((HALO, WIDE), BF16)
        vl[top : top + HALO, :] = jnp.zeros((HALO, WIDE), BF16)
    chain_step(1, 3, ivar_own)

    def own_stage(j, carry):
        at = pl.ds(pl.multiple_of(j * THIRD, S), THIRD)
        for rt in range(BR):
            here = slice(rt * S, rt * S + LEN)
            own_rows[rt * LEN : rt * LEN + LEN, at] = dot3((full_h[...], full_l[...]), (vh[here, at], vl[here, at]))
        return carry

    lax.fori_loop(0, 3, own_stage, 0)

    @pl.when(has_before)
    def _():
        halo_copy(0).wait_recv()

    @pl.when(has_next)
    def _():
        halo_copy(1).wait_recv()

    for rt, top in enumerate((0, HALO + BR * S)):
        high, low = split(image[top : top + HALO, :])
        for k, part in enumerate((high, low, high)):
            edges[rt, k * HALO : k * HALO + HALO, :] = part

    def edge_stage(j, carry):
        at = pl.ds(pl.multiple_of(j * THIRD, S), THIRD)
        for rt, table in enumerate((edge_first, edge_last)):
            there = slice(rt * LEN, rt * LEN + LEN)
            out = own_rows[there, at] + jnp.dot(table[...], edges[rt, :, at], preferred_element_type=F32)
            fxh[there, at], fxl[there, at] = split(out)
        return carry

    lax.fori_loop(0, 3, edge_stage, 0)

    def tile(bc):
        at = pl.ds(pl.multiple_of(bc * S, S), LEN)
        kcc, kcs = spec[:S, :S], spec[:S, S:]
        ksc, kss = spec[S:, :S], spec[S:, S:]
        for rt in range(BR):
            there = slice(rt * LEN, rt * LEN + LEN)
            freq = dot3((fxh[there, at], fxl[there, at]), (fullt_h[...], fullt_l[...]))
            xcc, xcs = freq[:S, :S], freq[:S, S:]
            xsc, xss = freq[S:, :S], freq[S:, S:]
            ycc = (xcc * kcc - xcs * kcs) - (xsc * ksc - xss * kss)
            ycs = (xcc * kcs + xcs * kcc) - (xsc * kss + xss * ksc)
            ysc = (xcc * ksc - xcs * kss) + (xsc * kcc - xss * kcs)
            yss = (xcc * kss + xcs * ksc) + (xsc * kcs + xss * kcc)
            prod = jnp.concatenate(
                [jnp.concatenate([ycc, ycs], axis=1), jnp.concatenate([ysc, yss], axis=1)], axis=0)
            back = dot3(split(prod), (mid_h[...], mid_l[...]))
            matched = dot3((midt_h[...], midt_l[...]), split(back))
            numer[rt, bc] = canvas[1, rt * BC + bc] * matched

    def numer_own(quarter, chunk):
        return numer[quarter // 2, chunk, quarter % 2 * PART : quarter % 2 * PART + PART, :]

    def tile_step(k, carry):
        near = (k + 1) // 2
        tile((v + 4 + jnp.where(k % 2 == 0, near, VISITS - near)) % VISITS)

        @pl.when(k == 0)
        def _():
            chain_first(0, numer_own)

        for step in (1, 2, 3):
            @pl.when(k == 2 * step)
            def _(step=step):
                chain_step(0, step, numer_own)

        return carry

    lax.fori_loop(0, VISITS, tile_step, 0)
    for quarter in range(4):
        weight_ref[quarter * PART : quarter * PART + PART, :] = chain_last(1, quarter, ivar_own)
    for quarter in range(4):
        coadd_ref[quarter * PART : quarter * PART + PART, :] = chain_last(0, quarter, numer_own)

    def drain(n, carry):
        route, j = n % 2, n // 2
        id_copy(route, j).wait_send()
        line_copy(0, route, j).wait_send()
        line_copy(1, route, j).wait_send()
        return carry

    lax.fori_loop(2, 16, drain, 0)
    for plane in (0, 1):
        for route in (0, 1):
            for m in range(6):
                pass_copy(plane, route, m).wait_send()
    for what in (0, 1):
        for direction in (0, 1):
            for step in (0, 1, 2, 3):
                for quarter in range(4):
                    if step > 0 or quarter // 2 == direction:
                        chain_copy(what, direction, step, quarter).wait_send()

    @pl.when(has_next)
    def _():
        halo_copy(0).wait_send()

    @pl.when(has_before)
    def _():
        halo_copy(1).wait_send()


def on_device(piece_flux, piece_ivar, warp_rows, warp_cols, piece_owner, piece_slot, piece_extent, basis, coeffs):
    owner = piece_owner.reshape(PIECES)
    order = jnp.arange(PIECES, dtype=jnp.int32)
    hit = owner[:, None] == jnp.arange(OWNERS, dtype=jnp.int32)[None, :]
    first = jnp.min(jnp.where(hit, order[:, None], PIECES), axis=0)
    last = jnp.max(jnp.where(hit, order[:, None], -1), axis=0)
    shape = (PIECES, S, S)
    vmem = pl.BlockSpec(memory_space=pltpu.VMEM)
    smem = pl.BlockSpec(memory_space=pltpu.SMEM)
    hbm = pl.BlockSpec(memory_space=pl.ANY)
    tables = dft_tables()
    dma = pltpu.SemaphoreType.DMA
    numerator, weight = pl.pallas_call(
        kernel,
        out_shape=[jax.ShapeDtypeStruct((BR * S, S), F32)] * 2,
        in_specs=[smem] * 5 + [hbm] * (4 + TABLES),
        out_specs=[vmem, vmem],
        scratch_shapes=[pltpu.VMEM(basis.shape, F32)]
        + [pltpu.VMEM(t.shape, BF16) for t in tables]
        + [pltpu.VMEM(shape, F32)] * 4
        + [
            pltpu.VMEM((2, 2, 8, 4, CAP, PART, S), F32),
            pltpu.VMEM((2, 2, 8, 4, CAP, PART, S), F32),
            pltpu.VMEM((2, 8, 8, S), F32),
            pltpu.VMEM((2, 8, 8, S), F32),
            pltpu.VMEM((2, 2, 4, BLOCKS, PART, S), F32),
            pltpu.VMEM((2, 2, 2, BLOCKS // 2, PART, S), F32),
            pltpu.VMEM((2, 2, 2, BLOCKS, PART, S), F32),
            pltpu.VMEM((2, BLOCKS, S, S), F32),
            pltpu.VMEM((TALL, WIDE), F32),
            pltpu.VMEM((TALL, WIDE), BF16),
            pltpu.VMEM((TALL, WIDE), BF16),
            pltpu.VMEM((BR * LEN, WIDE), BF16),
            pltpu.VMEM((BR * LEN, WIDE), BF16),
            pltpu.VMEM((LEN, LEN), F32),
            pltpu.VMEM((BR, BC, S, S), F32),
            pltpu.VMEM((2, 2, 4, 4, PART, S), F32),
            pltpu.VMEM((2, 2, 4, 4, PART, S), F32),
            dma((16,)),
            dma((2, 8)),
            dma((2, 8)),
            dma((2, 2, 8)),
            dma((2, 2, 8)),
            dma((2, 2, 6)),
            dma((2, 2, 6)),
            dma((2, 2, 4, 4)),
            dma((2, 2, 4, 4)),
            dma((2,)),
            dma((2,)),
            dma((TABLES,)),
            pltpu.VMEM((BR * LEN, WIDE), F32),
            pltpu.VMEM((BR, 3 * HALO, WIDE), BF16),
        ],
        compiler_params=pltpu.CompilerParams(
            collective_id=0, has_side_effects=True, vmem_limit_bytes=60 * 1024 * 1024
        ),
        name="coadd",
    )(
        first, last, piece_slot.reshape(PIECES), piece_extent.reshape(PIECES, 2).T, coeffs.reshape(4),
        piece_flux.reshape(shape), piece_ivar.reshape(shape), warp_rows.reshape(shape), warp_cols.reshape(shape),
        basis, *[jnp.asarray(t) for t in tables],
    )
    return numerator / jnp.maximum(weight, 1.0), jnp.maximum(weight, 0.0)


def solution(mesh):
    piece = P("visit", "bulk", None, None, None)
    return jax.shard_map(
        on_device,
        mesh=mesh,
        in_specs=(piece, piece, piece, piece, P("visit", "bulk", None, None), P("visit", "bulk", None),
                  P("visit", "bulk", None, None), P(), P("visit", None)),
        out_specs=(P("bulk", "visit"), P("bulk", "visit")),
        check_vma=False,
    )
```
